32 devices in a mesh: gx: 2 (over x), gy: 4 (over y, core), gz: 4 (over z).
Axes of the slice: x: 2, y: 2, z: 4, core: 2. Of those that a mesh axis runs over, the one named last changes fastest.
Arguments:
- displacement: float32 [3, 16, 32, 512], P(None, 'gx', 'gz', 'gy'), may hold values from -0.1 to 0.1
- velocity: float32 [3, 16, 32, 512], P(None, 'gx', 'gz', 'gy'), may hold values from -0.4 to 0.4
- body_force: float32 [3, 16, 32, 512], P(None, 'gx', 'gz', 'gy'), may hold values from -4 to 4
- broken: int32 [12, 16, 32, 512], P(None, 'gx', 'gz', 'gy'), may hold values from 0 to 1073741823
Outputs:
- new_displacement: float32 [3, 16, 32, 512], P(None, 'gx', 'gz', 'gy')
- new_velocity: float32 [3, 16, 32, 512], P(None, 'gx', 'gz', 'gy')
- new_acceleration: float32 [3, 16, 32, 512], P(None, 'gx', 'gz', 'gy')
- strain_energy: float32 [], replicated
The draws below stay inside these ranges and needn't reach their ends.
All inputs are finite; a program needn't handle non-finite values.
Results may differ from the reference program's by a relative error of at most 0.0003.
Values sent between devices are 32-bit elements; how exact they have to be, the bound alone decides.
A program may use at most 128 MiB of HBM per device.

```python
import math
import jax
import jax.numpy as jnp
from jax import lax

CX = 8
WORDS = 12
NX = 16
NZ = 32
NY = 512


def draw_displacement(key, part):
    key_noise = jax.random.fold_in(key, 11)
    along_x = (jnp.arange(NX, dtype=jnp.float32) + 0.5) / NX
    noise = jax.random.normal(key_noise, (3, NX, NZ, NY), jnp.float32)
    values = noise * (0.03 * (0.5 + along_x))[None, :, None, None]
    return jnp.clip(values, -0.1, 0.1)


def place_ends(result, own_key, low, high):
    longest = result.shape.index(max(result.shape))
    spots = []
    for shift in (0, 1):
        where = [jax.random.randint(jax.random.fold_in(own_key, axis), (), 0, length) for axis, length in enumerate(result.shape)]
        where[longest] = (where[longest] + shift) % result.shape[longest]
        spots.append(tuple(where))
    return result.at[spots[0]].set(low).at[spots[1]].set(high)


def block_levels(own_key, dims, split, least, high):
    factor_of, own = 1.0, jax.random.fold_in(own_key, 6)
    for axis_at, blocks in split:
        heights = jnp.exp(jax.random.uniform(jax.random.fold_in(own, axis_at), (blocks,), jnp.float32, least / len(split), high / len(split)))
        factor_of = factor_of * jnp.repeat(heights, dims[axis_at] // blocks).reshape([-1 if axis == axis_at else 1 for axis in range(len(dims))])
    return factor_of


def bell_draw(own_key, shape, width, most, split=(), held_as=jnp.bfloat16):
    entries = jax.random.normal(own_key, shape, jnp.float32) * width
    if len(split) > 0:
        entries = block_levels(own_key, shape, split, -0.22, 0.18) * entries
    return jnp.clip(entries, min=-most, max=most).astype(held_as)


def setup_inputs(seed: int = 0) -> dict:
    seeds = jax.random.split(jax.random.key(seed), 5)
    displacement = draw_displacement(jax.random.fold_in(seeds[4], 71), 0)
    velocity = bell_draw(seeds[1], (3, NX, NZ, NY), 0.15, 0.4, ((1, 2), (2, 4), (3, 4)), jnp.float32)
    body_force = bell_draw(seeds[2], (3, NX, NZ, NY), 1.0, 4.0, ((1, 2), (2, 4), (3, 4)), jnp.float32)
    broken = place_ends(jax.random.randint(seeds[3], (WORDS, NX, NZ, NY), 0, 1073741824), jax.random.fold_in(seeds[3], 1), 0, 1073741823).astype(jnp.int32)
    return dict(displacement=displacement, velocity=velocity, body_force=body_force, broken=broken)


TIME_STEP = 0.05
MICRO_MODULUS = 4.0
BITS_PER_WORD = 30
OFFSET_LIST = tuple(((step_x, step_z, step_y) for step_x in range(-3, 4) for step_z in range(-3, 4) for step_y in range(-3, 4) if (step_x, step_z, step_y) != (0, 0, 0)))

def bond_sum(extended, mask_block, depth_start, depth_total, row_count, depth_count, width_count, with_energy):
    center = extended[:, 3:3 + row_count, 3:3 + depth_count, 3:3 + width_count]
    depth_index = depth_start + jnp.arange(depth_count, dtype=jnp.int32)
    force_x = jnp.zeros(center.shape[1:], jnp.float32)
    force_z = jnp.zeros(center.shape[1:], jnp.float32)
    force_y = jnp.zeros(center.shape[1:], jnp.float32)
    energy = jnp.zeros(center.shape[1:], jnp.float32)
    for bond_index, (step_x, step_z, step_y) in enumerate(OFFSET_LIST):
        neighbour = extended[:, 3 + step_x:3 + step_x + row_count, 3 + step_z:3 + step_z + depth_count, 3 + step_y:3 + step_y + width_count]
        relative = neighbour - center
        bond_x = relative[0] + step_x
        bond_z = relative[1] + step_z
        bond_y = relative[2] + step_y
        length = jnp.sqrt(bond_x * bond_x + bond_z * bond_z + bond_y * bond_y)
        rest_length = math.sqrt(step_x * step_x + step_z * step_z + step_y * step_y)
        influence = math.exp(-rest_length * rest_length / 9.0)
        stretch = (length - rest_length) / rest_length
        broken_bit = jnp.right_shift(mask_block[bond_index // BITS_PER_WORD], bond_index % BITS_PER_WORD) & 1
        inside = (depth_index + step_z >= 0) & (depth_index + step_z < depth_total)
        intact = jnp.where(inside[None, :, None], 1 - broken_bit, 0).astype(jnp.float32)
        factor = intact * (MICRO_MODULUS * influence) * stretch / length
        force_x = force_x + factor * bond_x
        force_z = force_z + factor * bond_z
        force_y = force_y + factor * bond_y
        if with_energy:
            energy = energy + intact * (0.25 * MICRO_MODULUS * influence * rest_length) * stretch * stretch
    return (jnp.stack([force_x, force_z, force_y]), jnp.sum(energy))

def slab_forces(field_in, broken, with_energy):
    padded = jnp.pad(field_in, ((0, 0), (3, 3), (3, 3), (3, 3)), mode='wrap')
    starts = jnp.arange(NX // CX, dtype=jnp.int32) * CX

    def block_force(first_row):
        first_row = first_row.astype(jnp.int32)
        anchor = jnp.zeros((), jnp.int32)
        extended = lax.dynamic_slice(padded, (anchor, first_row, anchor, anchor), (3, CX + 6, NZ + 6, NY + 6))
        mask_block = lax.dynamic_slice(broken, (anchor, first_row, anchor, anchor), (WORDS, CX, NZ, NY))
        return bond_sum(extended, mask_block, 0, NZ, CX, NZ, NY, with_energy)
    pieces, energies = lax.map(block_force, starts)
    forces = jnp.moveaxis(pieces, 0, 1).reshape(3, NX, NZ, NY)
    return (forces, jnp.sum(energies))

def reference(displacement, velocity, body_force, broken):
    first_force, unused = slab_forces(displacement, broken, False)
    first_acceleration = first_force + body_force
    new_displacement = displacement + TIME_STEP * velocity + 0.5 * TIME_STEP * TIME_STEP * first_acceleration
    second_force, energy = slab_forces(new_displacement, broken, True)
    new_acceleration = second_force + body_force
    new_velocity = velocity + 0.5 * TIME_STEP * (first_acceleration + new_acceleration)
    strain_energy = energy / jnp.float32(NX * NY)
    return (new_displacement, new_velocity, new_acceleration, strain_energy)
```

```python
import functools
import math

import jax
import jax.numpy as jnp
from jax import lax
from jax.experimental import pallas as pl
from jax.experimental.pallas import tpu as pltpu
from jax.sharding import PartitionSpec as P

TIME_STEP = 0.05
MICRO_MODULUS = 4.0
BITS_PER_WORD = 30
W = 3
REACH = range(-W, W + 1)
BONDS = tuple(
    (p, q, r) for p in REACH for q in REACH for r in REACH if (p, q, r) != (0, 0, 0)
)
INDEX = {bond: k for k, bond in enumerate(BONDS)}
WORD_COUNT = -(-len(BONDS) // BITS_PER_WORD)


def extended(block, axis, dim):
    count = lax.axis_size(axis)
    forward = [(i, (i + 1) % count) for i in range(count)]
    backward = [(t, s) for s, t in forward]
    low = lax.ppermute(
        lax.slice_in_dim(block, block.shape[dim] - W, None, axis=dim), axis, forward
    )
    high = lax.ppermute(lax.slice_in_dim(block, 0, W, axis=dim), axis, backward)
    return low, high


def depth_bits(shape, depth_start, depth_total):
    depth = lax.broadcasted_iota(jnp.int32, shape, 0) + depth_start
    words = [jnp.zeros(shape, jnp.int32) for _ in range(WORD_COUNT)]
    for q in REACH:
        if q == 0:
            continue
        outside = (depth + q < 0) | (depth + q >= depth_total)
        for w in range(WORD_COUNT):
            bits = 0
            for (p, q2, r), k in INDEX.items():
                if q2 == q and k // BITS_PER_WORD == w:
                    bits |= 1 << (k % BITS_PER_WORD)
            if bits:
                words[w] = words[w] | jnp.where(outside, bits, 0)
    return words


def store_masks(broken_ref, mask_ref, outside_ref, depth_start, depth_total):
    rows = broken_ref.shape[1]
    for w, word in enumerate(depth_bits(broken_ref.shape[2:], depth_start, depth_total)):
        outside_ref[w] = word

    def body(x, carry):
        for w in range(WORD_COUNT):
            word = broken_ref[w, x] | outside_ref[w]
            for k in range(w * BITS_PER_WORD, min(len(BONDS), (w + 1) * BITS_PER_WORD)):
                p, q, r = BONDS[k]
                weight = MICRO_MODULUS * math.exp(-(p * p + q * q + r * r) / 9.0)
                bit = word & (1 << (k % BITS_PER_WORD))
                mask_ref[k, x] = jnp.where(bit == 0, jnp.float32(weight), jnp.float32(0.0))
        return carry

    lax.fori_loop(0, rows, body, 0)


def shifted_rows(a, b, lane, e_ref, c, x):
    width = a.shape[1]
    depth = a.shape[0]
    for r in REACH:
        if r == 0:
            tile = a
        elif r > 0:
            tile = pltpu.roll(jnp.where(lane < r, b, a), width - r, 1)
        else:
            tile = pltpu.roll(jnp.where(lane >= width + r, b, a), -r, 1)
        if c == 2 and r != 0:
            tile = tile + float(r)
        e_ref[r + W, c, x, 0:depth] = tile


def bond_rows(x, steps, e_ref, mask_ref, depth, with_energy):
    center = [e_ref[W, c, x + W, W : W + depth] for c in range(3)]
    force = [jnp.zeros_like(center[0]) for _ in range(3)]
    energy = jnp.zeros_like(center[0])
    for p in steps:
        center_x = center[0] - float(p)
        for q in REACH:
            center_z = center[1] - float(q)
            for r in REACH:
                if (p, q, r) == (0, 0, 0):
                    continue
                k = INDEX[(p, q, r)]
                rest = math.sqrt(p * p + q * q + r * r)
                nb = [
                    e_ref[r + W, c, x + (W + p), W + q : W + q + depth] for c in range(3)
                ]
                bx = nb[0] - center_x
                bz = nb[1] - center_z
                by = nb[2] - center[2]
                square = bx * bx + bz * bz + by * by
                h = jnp.float32(1.0 / rest) - lax.rsqrt(square)
                g = mask_ref[k, x] * h
                force[0] = force[0] + g * bx
                force[1] = force[1] + g * bz
                force[2] = force[2] + g * by
                if with_energy:
                    energy = energy + (g * jnp.float32(0.25 * rest)) * (h * square)
    return force, energy


def pass_kernel(
    depth_total, with_energy, a_ref, b_ref, broken_ref, force_ref, energy_ref,
    e_ref, mask_ref, outside_ref,
):
    rows, depth = broken_ref.shape[1], broken_ref.shape[2]
    width = a_ref.shape[3]
    depth_start = lax.axis_index("gz") * depth
    store_masks(broken_ref, mask_ref, outside_ref, depth_start, depth_total)
    lane = lax.broadcasted_iota(jnp.int32, a_ref.shape[2:], 1)

    def fill(x, carry):
        for c in range(3):
            shifted_rows(a_ref[c, x], b_ref[c, x], lane, e_ref, c, x)
        return carry

    lax.fori_loop(0, rows + 2 * W, fill, 0)
    energy_ref[...] = jnp.zeros_like(energy_ref)

    def body(x, carry):
        force, energy = bond_rows(x, REACH, e_ref, mask_ref, depth, with_energy)
        for c in range(3):
            force_ref[c, x] = force[c]
        if with_energy:
            energy_ref[...] += energy
        return carry

    lax.fori_loop(0, rows, body, 0)


def bond_sum(field, broken, with_energy):
    _, rows, depth, width = field.shape
    depth_total = depth * lax.axis_size("gz")
    low, high = extended(field, "gx", 1)
    field = jnp.concatenate([low, field, high], axis=1)
    low, high = extended(field, "gz", 2)
    field = jnp.concatenate([low, field, high], axis=2)
    low, high = extended(field, "gy", 3)
    sides = jnp.concatenate(
        [high, jnp.zeros(field.shape[:3] + (width - 2 * W,), field.dtype), low], axis=3
    )
    padded = -(-(depth + 2 * W) // 8) * 8
    return pl.pallas_call(
        functools.partial(pass_kernel, depth_total, with_energy),
        out_shape=(
            jax.ShapeDtypeStruct((3, rows, depth, width), jnp.float32),
            jax.ShapeDtypeStruct((depth, width), jnp.float32),
        ),
        in_specs=[pl.BlockSpec(memory_space=pltpu.VMEM)] * 3,
        out_specs=(pl.BlockSpec(memory_space=pltpu.VMEM),) * 2,
        scratch_shapes=[
            pltpu.VMEM((2 * W + 1, 3, rows + 2 * W, padded, width), jnp.float32),
            pltpu.VMEM((len(BONDS), rows, depth, width), jnp.float32),
            pltpu.VMEM((WORD_COUNT, depth, width), jnp.int32),
        ],
        compiler_params=pltpu.CompilerParams(vmem_limit_bytes=48 * 1024 * 1024),
    )(field, sides, broken)


def per_device(displacement, velocity, body_force, broken):
    rows, width = displacement.shape[1], displacement.shape[3]
    first_force, unused = bond_sum(displacement, broken, False)
    first_acceleration = first_force + body_force
    new_displacement = (
        displacement + TIME_STEP * velocity + 0.5 * TIME_STEP * TIME_STEP * first_acceleration
    )
    second_force, local_energy = bond_sum(new_displacement, broken, True)
    new_acceleration = second_force + body_force
    new_velocity = velocity + 0.5 * TIME_STEP * (first_acceleration + new_acceleration)
    total_energy = lax.psum(jnp.sum(local_energy), ("gx", "gy", "gz"))
    area = rows * lax.axis_size("gx") * width * lax.axis_size("gy")
    strain_energy = total_energy / jnp.float32(area)
    return (new_displacement, new_velocity, new_acceleration, strain_energy)


def solution(mesh):
    spec = P(None, "gx", "gz", "gy")
    return jax.shard_map(
        per_device,
        mesh=mesh,
        in_specs=(spec,) * 4,
        out_specs=(spec, spec, spec, P()),
        check_vma=False,
    )
```

```python
import functools
import math

import jax
import jax.numpy as jnp
from jax import lax
from jax.experimental import pallas as pl
from jax.experimental.pallas import tpu as pltpu
from jax.sharding import PartitionSpec as P

TIME_STEP = 0.05
MICRO_MODULUS = 4.0
BITS_PER_WORD = 30
W = 3
REACH = range(-W, W + 1)
BONDS = tuple(
    (p, q, r) for p in REACH for q in REACH for r in REACH if (p, q, r) != (0, 0, 0)
)
INDEX = {bond: k for k, bond in enumerate(BONDS)}
WORD_COUNT = -(-len(BONDS) // BITS_PER_WORD)


def extended(block, axis, dim):
    count = lax.axis_size(axis)
    forward = [(i, (i + 1) % count) for i in range(count)]
    backward = [(t, s) for s, t in forward]
    low = lax.ppermute(
        lax.slice_in_dim(block, block.shape[dim] - W, None, axis=dim), axis, forward
    )
    high = lax.ppermute(lax.slice_in_dim(block, 0, W, axis=dim), axis, backward)
    return low, high


def depth_bits(shape, depth_start, depth_total):
    depth = lax.broadcasted_iota(jnp.int32, shape, 0) + depth_start
    words = [jnp.zeros(shape, jnp.int32) for _ in range(WORD_COUNT)]
    for q in REACH:
        if q == 0:
            continue
        outside = (depth + q < 0) | (depth + q >= depth_total)
        for w in range(WORD_COUNT):
            bits = 0
            for (p, q2, r), k in INDEX.items():
                if q2 == q and k // BITS_PER_WORD == w:
                    bits |= 1 << (k % BITS_PER_WORD)
            if bits:
                words[w] = words[w] | jnp.where(outside, bits, 0)
    return words


def store_masks(broken_ref, mask_ref, outside_ref, depth_start, depth_total):
    rows = broken_ref.shape[1]
    for w, word in enumerate(depth_bits(broken_ref.shape[2:], depth_start, depth_total)):
        outside_ref[w] = word

    def body(x, carry):
        for w in range(WORD_COUNT):
            word = broken_ref[w, x] | outside_ref[w]
            for k in range(w * BITS_PER_WORD, min(len(BONDS), (w + 1) * BITS_PER_WORD)):
                p, q, r = BONDS[k]
                weight = MICRO_MODULUS * math.exp(-(p * p + q * q + r * r) / 9.0)
                bit = word & (1 << (k % BITS_PER_WORD))
                mask_ref[k, x] = jnp.where(bit == 0, jnp.float32(weight), jnp.float32(0.0))
        return carry

    lax.fori_loop(0, rows, body, 0)


def shifted_rows(a, b, lane, e_ref, c, x):
    width = a.shape[1]
    depth = a.shape[0]
    for r in REACH:
        if r == 0:
            tile = a
        elif r > 0:
            tile = pltpu.roll(jnp.where(lane < r, b, a), width - r, 1)
        else:
            tile = pltpu.roll(jnp.where(lane >= width + r, b, a), -r, 1)
        if c == 2 and r != 0:
            tile = tile + float(r)
        e_ref[r + W, c, x, 0:depth] = tile


def bond_rows(x, steps, e_ref, mask_ref, depth, with_energy):
    center = [e_ref[W, c, x + W, W : W + depth] for c in range(3)]
    force = [jnp.zeros_like(center[0]) for _ in range(3)]
    energy = jnp.zeros_like(center[0])
    for p in steps:
        center_x = center[0] - float(p)
        for q in REACH:
            center_z = center[1] - float(q)
            for r in REACH:
                if (p, q, r) == (0, 0, 0):
                    continue
                k = INDEX[(p, q, r)]
                rest = math.sqrt(p * p + q * q + r * r)
                nb = [
                    e_ref[r + W, c, x + (W + p), W + q : W + q + depth] for c in range(3)
                ]
                bx = nb[0] - center_x
                bz = nb[1] - center_z
                by = nb[2] - center[2]
                square = bx * bx + bz * bz + by * by
                h = jnp.float32(1.0 / rest) - lax.rsqrt(square)
                g = mask_ref[k, x] * h
                force[0] = force[0] + g * bx
                force[1] = force[1] + g * bz
                force[2] = force[2] + g * by
                if with_energy:
                    energy = energy + (g * jnp.float32(0.25 * rest)) * (h * square)
    return force, energy


def pass_kernel(
    depth_total, with_energy, a_ref, b_ref, broken_ref, force_ref, energy_ref,
    e_ref, mask_ref, outside_ref,
):
    rows, depth = broken_ref.shape[1], broken_ref.shape[2]
    width = a_ref.shape[3]
    depth_start = lax.axis_index("gz") * depth
    store_masks(broken_ref, mask_ref, outside_ref, depth_start, depth_total)
    lane = lax.broadcasted_iota(jnp.int32, a_ref.shape[2:], 1)

    def fill(x, carry):
        for c in range(3):
            shifted_rows(a_ref[c, x], b_ref[c, x], lane, e_ref, c, x)
        return carry

    lax.fori_loop(0, rows + 2 * W, fill, 0)
    energy_ref[...] = jnp.zeros_like(energy_ref)

    def body(x, carry):
        force, energy = bond_rows(x, REACH, e_ref, mask_ref, depth, with_energy)
        for c in range(3):
            force_ref[c, x] = force[c]
        if with_energy:
            energy_ref[...] += energy
        return carry

    lax.fori_loop(0, rows, body, 0)


def bond_sum(field, broken, with_energy):
    _, rows, depth, width = field.shape
    depth_total = depth * lax.axis_size("gz")
    low, high = extended(field, "gx", 1)
    field = jnp.concatenate([low, field, high], axis=1)
    low, high = extended(field, "gz", 2)
    field = jnp.concatenate([low, field, high], axis=2)
    low, high = extended(field, "gy", 3)
    sides = jnp.concatenate(
        [high, jnp.zeros(field.shape[:3] + (width - 2 * W,), field.dtype), low], axis=3
    )
    padded = -(-(depth + 2 * W) // 8) * 8
    return pl.pallas_call(
        functools.partial(pass_kernel, depth_total, with_energy),
        out_shape=(
            jax.ShapeDtypeStruct((3, rows, depth, width), jnp.float32),
            jax.ShapeDtypeStruct((depth, width), jnp.float32),
        ),
        in_specs=[pl.BlockSpec(memory_space=pltpu.VMEM)] * 3,
        out_specs=(pl.BlockSpec(memory_space=pltpu.VMEM),) * 2,
        scratch_shapes=[
            pltpu.VMEM((2 * W + 1, 3, rows + 2 * W, padded, width), jnp.float32),
            pltpu.VMEM((len(BONDS), rows, depth, width), jnp.float32),
            pltpu.VMEM((WORD_COUNT, depth, width), jnp.int32),
        ],
        compiler_params=pltpu.CompilerParams(vmem_limit_bytes=48 * 1024 * 1024),
    )(field, sides, broken)


AXES = ("gx", "gy", "gz")


def sum_kernel(counts, tile_ref, total_ref, *scratch):
    slots, (send_sem, recv_sem) = scratch[: len(AXES)], scratch[len(AXES) :]
    barrier = pltpu.get_barrier_semaphore()
    peers = 0
    for axis, count in zip(AXES, counts):
        me = lax.axis_index(axis)
        for d in range(1, count):
            pl.semaphore_signal(
                barrier,
                inc=1,
                device_id={axis: lax.rem(me + d, count)},
                device_id_type=pl.DeviceIdType.MESH,
            )
            peers += 1
    pl.semaphore_wait(barrier, peers)
    at = 0
    value = tile_ref[...]
    for slot, axis, count in zip(slots, AXES, counts):
        me = lax.axis_index(axis)
        slot[me] = value
        copies = []
        for d in range(1, count):
            copy = pltpu.make_async_remote_copy(
                src_ref=slot.at[me],
                dst_ref=slot.at[me],
                send_sem=send_sem.at[at],
                recv_sem=recv_sem.at[at],
                device_id={axis: lax.rem(me + d, count)},
                device_id_type=pl.DeviceIdType.MESH,
            )
            copy.start()
            copies.append(copy)
            at += 1
        for copy in copies:
            copy.wait()
        value = slot[0]
        for i in range(1, count):
            value = value + slot[i]
    total_ref[...] = value


def mesh_sum(tile):
    counts = tuple(lax.axis_size(axis) for axis in AXES)
    peers = sum(counts) - len(counts)
    return pl.pallas_call(
        functools.partial(sum_kernel, counts),
        out_shape=jax.ShapeDtypeStruct(tile.shape, tile.dtype),
        in_specs=[pl.BlockSpec(memory_space=pltpu.VMEM)],
        out_specs=pl.BlockSpec(memory_space=pltpu.VMEM),
        scratch_shapes=[pltpu.VMEM((count,) + tile.shape, tile.dtype) for count in counts]
        + [pltpu.SemaphoreType.DMA((peers,)), pltpu.SemaphoreType.DMA((peers,))],
        compiler_params=pltpu.CompilerParams(collective_id=0, has_side_effects=True),
    )(tile)


def per_device(displacement, velocity, body_force, broken):
    rows, width = displacement.shape[1], displacement.shape[3]
    first_force, unused = bond_sum(displacement, broken, False)
    first_acceleration = first_force + body_force
    new_displacement = (
        displacement + TIME_STEP * velocity + 0.5 * TIME_STEP * TIME_STEP * first_acceleration
    )
    second_force, local_energy = bond_sum(new_displacement, broken, True)
    new_acceleration = second_force + body_force
    new_velocity = velocity + 0.5 * TIME_STEP * (first_acceleration + new_acceleration)
    total_energy = jnp.sum(mesh_sum(local_energy))
    area = rows * lax.axis_size("gx") * width * lax.axis_size("gy")
    strain_energy = total_energy / jnp.float32(area)
    return (new_displacement, new_velocity, new_acceleration, strain_energy)


def solution(mesh):
    spec = P(None, "gx", "gz", "gy")
    return jax.shard_map(
        per_device,
        mesh=mesh,
        in_specs=(spec,) * 4,
        out_specs=(spec, spec, spec, P()),
        check_vma=False,
    )
```
